32 devices in a mesh: dp: 16 (over z, x, core), tensor: 2 (over y).
Axes of the slice: x: 2, y: 2, z: 4, core: 2. Of those that a mesh axis runs over, the one named last changes fastest.
Arguments:
- stream: bfloat16 [4, 16384, 768], P(None, ('dp', 'tensor')), may hold values from -6 to 6
- bounds: int32 [4, 16, 2], P(None, 'dp'), may hold values from 256 to 1024, as said below
- prescale: bfloat16 [768], P(('dp', 'tensor')), may hold values from 0.099609375 to 1.8984375
- expansion: bfloat16 [768, 2, 1536], P('dp', None, 'tensor'), may hold values from -0.21875 to 0.21875
- timestep: bfloat16 [768, 24], P('dp', 'tensor'), may hold values from -0.21875 to 0.21875
- selection: bfloat16 [768, 256], P(('dp', 'tensor')), may hold values from -0.21875 to 0.21875
- kernels: bfloat16 [24, 256], P('tensor', 'dp'), may hold values from -3 to 3
- biases: bfloat16 [24, 64], P('tensor', 'dp'), may hold values from -0.5 to 0.5
- stencil: bfloat16 [256, 4], P(('dp', 'tensor')), may hold values from -3 to 3
- baseline: bfloat16 [256], P(('dp', 'tensor')), may hold values from -0.5 to 0.5
- offset: bfloat16 [24], P('tensor'), may hold values from -6.875 to -2.296875
- decays: bfloat16 [24], P('tensor'), may hold values from 0 to 2.765625
- passthrough: bfloat16 [24], P('tensor'), may hold values from 0.5 to 1.5
- rescale: bfloat16 [24, 64], P('tensor', 'dp'), may hold values from 0.099609375 to 1.8984375
- readout: bfloat16 [1536, 768], P('tensor', 'dp'), may hold values from -0.15625 to 0.15625
- cotangent: bfloat16 [4, 16384, 768], P(None, ('dp', 'tensor')), may hold values from -6 to 6
Outputs:
- result: bfloat16 [4, 16384, 768], P(None, ('dp', 'tensor'))
- stream_gradient: bfloat16 [4, 16384, 768], P(None, ('dp', 'tensor'))
- prescale_gradient: float32 [768], P(('dp', 'tensor'))
- expansion_gradient: float32 [768, 2, 1536], P('dp', None, 'tensor')
- timestep_gradient: float32 [768, 24], P('dp', 'tensor')
- selection_gradient: float32 [768, 256], P(('dp', 'tensor'))
- kernels_gradient: float32 [24, 256], P('tensor', 'dp')
- biases_gradient: float32 [24, 64], P('tensor', 'dp')
- stencil_gradient: float32 [256, 4], P(('dp', 'tensor'))
- baseline_gradient: float32 [256], P(('dp', 'tensor'))
- offset_gradient: float32 [24], P('tensor')
- decays_gradient: float32 [24], P('tensor')
- passthrough_gradient: float32 [24], P('tensor')
- rescale_gradient: float32 [24, 64], P('tensor', 'dp')
- readout_gradient: float32 [1536, 768], P('tensor', 'dp')
The draws below stay inside these ranges and needn't reach their ends.
Inputs may be any that keep to these rules, and one draw needn't show every extreme that they name: bounds[m, s, 0] ends the slot's first sequence, which starts at position 0; positions from there up to bounds[m, s, 1] form a second sequence of 0 or at least 256 positions; positions after bounds[m, s, 1] are padding. In each micro-batch one slot is filled by one sequence of 1024 positions and another holds a single sequence of 256.
All inputs are finite; a program needn't handle non-finite values.
Results may differ from the reference program's by a relative error of at most 0.022.
Values may be sent and summed in bfloat16 or wider, within the bound.
A program may use at most 512 MiB of HBM per device.

```python
import jax
import jax.numpy as jnp
from jax import lax

WIDTH = 768
HEADS = 24
HEAD_DIM = 64
STATE = 128
TAPS = 4
STRETCH = 256
INNER = 1536
SLOT = 1024
MICRO = 4
SLOTS = 16
TOKENS = 16384


def draw_bounds(key, part):
    first_key, second_key, coin_key, pick_key, other_key = jax.random.split(key, 5)
    quarter = SLOT // 4
    first = jax.random.randint(first_key, (MICRO, SLOTS), quarter, SLOT + 1)
    room = SLOT - first
    second = jax.random.randint(second_key, (MICRO, SLOTS), quarter, jnp.maximum(room, quarter) + 1)
    coin = jax.random.randint(coin_key, (MICRO, SLOTS), 0, 2)
    second = jnp.where((room >= quarter) & (coin == 1), second, 0)
    full_slot = jax.random.randint(pick_key, (MICRO, 1), 0, SLOTS)
    short_slot = (full_slot + 1 + jax.random.randint(other_key, (MICRO, 1), 0, SLOTS - 1)) % SLOTS
    column = jnp.arange(SLOTS)[None, :]
    first = jnp.where(column == full_slot, SLOT, jnp.where(column == short_slot, quarter, first))
    second = jnp.where((column == full_slot) | (column == short_slot), 0, second)
    return jnp.stack([first, first + second], axis=-1).astype(jnp.int32)


def steps_of(rng, extent, cuts, least, high):
    level, own = 1.0, jax.random.fold_in(rng, 6)
    for dim, blocks in cuts:
        steps = jnp.exp(jax.random.uniform(jax.random.fold_in(own, dim), (blocks,), jnp.float32, least / len(cuts), high / len(cuts)))
        level = level * jnp.repeat(steps, extent[dim] // blocks).reshape([-1 if axis == dim else 1 for axis in range(len(extent))])
    return level


def bell_draw(key, shape, deviation, reach, cuts=(), kind=jnp.bfloat16):
    entries = jax.random.normal(key, shape, jnp.float32) * deviation
    if len(cuts) > 0:
        entries = steps_of(key, shape, cuts, -0.22, 0.18) * entries
    return jnp.clip(entries, min=-reach, max=reach).astype(kind)


def setup_inputs(seed: int = 0) -> dict:
    arg_keys = jax.random.split(jax.random.key(seed), 17)
    stream = bell_draw(arg_keys[0], (MICRO, TOKENS, WIDTH), 1.0, 6.0, ((1, 32),))
    bounds = draw_bounds(jax.random.fold_in(arg_keys[16], 71), 0)
    prescale = jnp.clip(1.0 + 0.18 * jax.random.normal(arg_keys[2], (WIDTH,), jnp.float32), 0.099609375, 1.8984375).astype(jnp.bfloat16)
    expansion = bell_draw(arg_keys[3], (WIDTH, 2, INNER), WIDTH ** -0.5, 0.21875, ((0, 16), (2, 2)))
    timestep = bell_draw(arg_keys[4], (WIDTH, HEADS), WIDTH ** -0.5, 0.21875, ((0, 16), (1, 2)))
    selection = bell_draw(arg_keys[5], (WIDTH, 2 * STATE), WIDTH ** -0.5, 0.21875, ((0, 32),))
    kernels = bell_draw(arg_keys[6], (HEADS, HEAD_DIM * TAPS), TAPS ** -0.5, 3.0, ((0, 2), (1, 16)))
    biases = jnp.clip(jax.random.uniform(arg_keys[7], (HEADS, HEAD_DIM), jnp.float32, -0.5, 0.5) * steps_of(arg_keys[7], (HEADS, HEAD_DIM), ((0, 2), (1, 16)), -0.4, 0.0), -0.5, 0.5).astype(jnp.bfloat16)
    stencil = bell_draw(arg_keys[8], (2 * STATE, TAPS), TAPS ** -0.5, 3.0, ((0, 32),))
    baseline = jnp.clip(jax.random.uniform(arg_keys[9], (2 * STATE,), jnp.float32, -0.5, 0.5) * steps_of(arg_keys[9], (2 * STATE,), ((0, 32),), -0.4, 0.0), -0.5, 0.5).astype(jnp.bfloat16)
    offset = jnp.clip(-6.875 + 4.578125 * jax.random.uniform(arg_keys[10], (HEADS,), jnp.float32) ** steps_of(arg_keys[10], (HEADS,), ((0, 2),), -0.2, 0.2), -6.875, -2.296875).astype(jnp.bfloat16)
    decays = jnp.clip(2.765625 * jax.random.uniform(arg_keys[11], (HEADS,), jnp.float32) ** steps_of(arg_keys[11], (HEADS,), ((0, 2),), -0.2, 0.2), 0.0, 2.765625).astype(jnp.bfloat16)
    passthrough = jnp.clip(0.5 + 1.0 * jax.random.uniform(arg_keys[12], (HEADS,), jnp.float32) ** steps_of(arg_keys[12], (HEADS,), ((0, 2),), -0.2, 0.2), 0.5, 1.5).astype(jnp.bfloat16)
    rescale = jnp.clip(1.0 + 0.18 * jax.random.normal(arg_keys[13], (HEADS, HEAD_DIM), jnp.float32), 0.099609375, 1.8984375).astype(jnp.bfloat16)
    readout = bell_draw(arg_keys[14], (INNER, WIDTH), INNER ** -0.5, 0.15625, ((0, 2), (1, 16)))
    cotangent = bell_draw(arg_keys[15], (MICRO, TOKENS, WIDTH), 1.0, 6.0, ((1, 32),))
    return {"stream": stream, "bounds": bounds, "prescale": prescale, "expansion": expansion, "timestep": timestep, "selection": selection, "kernels": kernels, "biases": biases, "stencil": stencil, "baseline": baseline, "offset": offset, "decays": decays, "passthrough": passthrough, "rescale": rescale, "readout": readout, "cotangent": cotangent}


@jax.custom_vjp
def low(v):
    return lax.optimization_barrier(v.astype(jnp.bfloat16)).astype(jnp.float32)

@jax.custom_vjp
def low_back(v):
    return v

def low_keep(v):
    return (low(v), None)

def low_pass(kept, grad):
    return (grad,)

def back_keep(v):
    return (v, None)

def back_low(kept, grad):
    return (low(grad),)
low.defvjp(low_keep, low_pass)
low_back.defvjp(back_keep, back_low)
epsilon = 1e-05
highest = lax.Precision.HIGHEST

def row_norm(rows, gain):
    return rows * lax.rsqrt(lax.optimization_barrier(jnp.mean(rows * rows, axis=-1, keepdims=True)) + epsilon) * gain

def segments(limits):
    position = jnp.arange(SLOT, dtype=jnp.int32)[None, :]
    first = limits[:, 0:1]
    used = limits[:, 1:2]
    segment = (position >= first).astype(jnp.int32) + (position >= used).astype(jnp.int32)
    live = (position < used).astype(jnp.float32)
    return (segment, live)

def mix_taps(signal, taps, shifts, segment):
    width = taps.shape[1]
    length = signal.shape[1]
    total = shifts + signal * taps[:, width - 1]
    for back in range(1, width):
        moved = jnp.pad(signal, ((0, 0), (back, 0), (0, 0)))[:, :length]
        earlier = jnp.pad(segment, ((0, 0), (back, 0)), constant_values=-1)[:, :length]
        same = (earlier == segment)[:, :, None]
        total = total + jnp.where(same, moved, 0.0) * taps[:, width - 1 - back]
    return jax.nn.silu(total)

def decay_table(cumulative, segment):
    length = cumulative.shape[1]
    order = jnp.arange(length)
    mask = (order[:, None] >= order[None, :])[None] & (segment[:, :, None] == segment[:, None, :])
    mask = mask[:, None]
    spread = jnp.transpose(cumulative, (0, 2, 1))
    gap = spread[:, :, :, None] - spread[:, :, None, :]
    return jnp.where(mask, jnp.exp(jnp.where(mask, gap, 0.0)), 0.0)

def carry_part(reader, entry, scaled, cumulative, segment):
    count = cumulative.shape[0]
    last = segment[:, -1:]
    weight = jnp.where((segment == last)[:, :, None], jnp.exp(cumulative[:, -1:, :] - cumulative), 0.0)
    states = jnp.einsum('cjn,cjhp->chnp', entry, scaled * weight[:, :, :, None], precision=highest)
    carry = states[0]
    pieces = [jnp.zeros_like(scaled[0])]
    for index in range(1, count):
        inside = (segment[index] == segment[index - 1, -1]).astype(cumulative.dtype)
        factor = jnp.exp(cumulative[index]) * inside[:, None]
        pieces.append(jnp.einsum('in,hnp->ihp', reader[index], carry, precision=highest) * factor[:, :, None])
        carry = carry * (jnp.exp(cumulative[index, -1]) * inside[-1])[:, None, None] + states[index]
    return jnp.stack(pieces)

def slot_scan(scaled, entry, reader, cumulative, segment):
    table = decay_table(cumulative, segment)
    inner = low_back(jnp.einsum('cin,cjn->cij', reader, entry, precision=highest))
    weights = low(inner[:, None] * table)
    diagonal = jnp.einsum('chij,cjhp->cihp', weights, scaled, precision=highest)
    return diagonal + carry_part(reader, entry, scaled, cumulative, segment)

def forward(params, stream_rows, segment, live):
    prescale, expansion, timestep, selection, kernels, biases, stencil, baseline, offset, decays, passthrough, rescale, readout = params
    slots = segment.shape[0]
    normed = low(row_norm(stream_rows, prescale))
    joined = jnp.concatenate([expansion.reshape(WIDTH, 2 * INNER), timestep], axis=1)
    projected = low_back(jnp.dot(normed, joined, precision=highest))
    gate = projected[:, :INNER]
    inner_in = projected[:, INNER:2 * INNER]
    step_raw = projected[:, 2 * INNER:]
    chosen = low(low_back(jnp.dot(normed, selection, precision=highest)))
    signal = jnp.concatenate([inner_in, chosen], axis=1).reshape(slots, SLOT, INNER + 2 * STATE)
    taps = jnp.concatenate([kernels.reshape(INNER, TAPS), stencil], axis=0)
    shifts = jnp.concatenate([biases.reshape(INNER), baseline])
    mixed = mix_taps(signal, taps, shifts, segment).reshape(slots * SLOT, INNER + 2 * STATE)
    convolved = mixed[:, :INNER].reshape(slots * SLOT, HEADS, HEAD_DIM)
    entry = low(mixed[:, INNER:INNER + STATE])
    reader = low(mixed[:, INNER + STATE:])
    step = jax.nn.softplus(step_raw + offset)
    rate = -jnp.exp(decays) * step
    scaled = low(convolved * step[:, :, None])
    block_shape = (slots, SLOT // STRETCH, STRETCH)
    cumulative = jnp.cumsum(rate.reshape(block_shape + (HEADS,)), axis=2)
    core = jax.vmap(slot_scan)(scaled.reshape(block_shape + (HEADS, HEAD_DIM)), entry.reshape(block_shape + (STATE,)), reader.reshape(block_shape + (STATE,)), cumulative, segment.reshape(block_shape))
    output = core.reshape(slots * SLOT, HEADS, HEAD_DIM) + passthrough[:, None] * convolved
    output = low_back(output.reshape(slots * SLOT, INNER))
    gated = output * jax.nn.silu(gate)
    lifted = row_norm(gated, rescale.reshape(INNER))
    mixer = jnp.dot(low(lifted), readout, precision=highest)
    return stream_rows + live.reshape(-1)[:, None] * mixer

def reference(stream, bounds, prescale, expansion, timestep, selection, kernels, biases, stencil, baseline, offset, decays, passthrough, rescale, readout, cotangent):
    params = tuple((item.astype(jnp.float32) for item in (prescale, expansion, timestep, selection, kernels, biases, stencil, baseline, offset, decays, passthrough, rescale, readout)))
    group = 4
    groups = MICRO * SLOTS // group
    stream_groups = stream.astype(jnp.float32).reshape(groups, group * SLOT, WIDTH)
    back_groups = cotangent.astype(jnp.float32).reshape(groups, group * SLOT, WIDTH)
    bound_groups = bounds.reshape(groups, group, 2)

    def visit(totals, inputs):
        rows, limits, back = inputs
        segment, live = segments(limits)
        value, pullback = jax.vjp(lambda weights, values: forward(weights, values, segment, live), params, rows)
        weight_grads, row_grads = pullback(back)
        totals = jax.tree.map(jnp.add, totals, weight_grads)
        return (totals, (value.astype(jnp.bfloat16), row_grads.astype(jnp.bfloat16)))
    zeros = jax.tree.map(jnp.zeros_like, params)
    totals, (result, stream_gradient) = lax.scan(visit, zeros, (stream_groups, bound_groups, back_groups))
    return (result.reshape(MICRO, TOKENS, WIDTH), stream_gradient.reshape(MICRO, TOKENS, WIDTH), totals[0], totals[1], totals[2], totals[3], totals[4], totals[5], totals[6], totals[7], totals[8], totals[9], totals[10], totals[11], totals[12])
```

```python
import functools

import jax
import jax.numpy as jnp
from jax import lax
from jax.experimental import pallas as pl
from jax.experimental.pallas import tpu as pltpu
from jax.sharding import PartitionSpec as P

WIDTH = 768
HEADS = 24
HEAD_DIM = 64
STATE = 128
TAPS = 4
INNER = 1536
SLOT = 1024
CHUNK = 128
LANES = 128
GROUP = 256
CHANNELS = INNER + 2 * STATE
EPS = 1e-05
BF = jnp.bfloat16
F32 = jnp.float32
VMEM_LIMIT = 56 * 1024 * 1024


def nn(a, b):
    return lax.dot_general(a, b, (((1,), (0,)), ((), ())), preferred_element_type=F32)


def nt(a, b):
    return lax.dot_general(a, b, (((1,), (1,)), ((), ())), preferred_element_type=F32)


def tn(a, b):
    return lax.dot_general(a, b, (((0,), (0,)), ((), ())), preferred_element_type=F32)


def exact_dot(a, b):
    return lax.dot_general(
        a, b, (((1,), (0,)), ((), ())), preferred_element_type=F32, precision=lax.Precision.HIGHEST
    )


def pieces(v):
    high = v.astype(BF)
    low = (v - high.astype(F32)).astype(BF)
    return high, low


def doubled(v):
    high, low = pieces(v)
    return (high.astype(F32) + pltpu.roll(low.astype(F32), HEADS, 1)).astype(BF)


def softplus(v):
    return jnp.maximum(v, 0.0) + jnp.log1p(jnp.exp(-jnp.abs(v)))


def sigmoid(v):
    return 1.0 / (1.0 + jnp.exp(-v))


def wide(column):
    return jnp.broadcast_to(column, (CHUNK, LANES))


def shifted(block, tail):
    full = jnp.concatenate([tail, block], axis=0)
    return [pltpu.roll(full, back, 0)[8:] for back in range(1, TAPS)]


def total_of(block, moved, masks, taps_ref, lanes):
    total = taps_ref[TAPS : TAPS + 1, lanes] + block * taps_ref[TAPS - 1 : TAPS, lanes]
    masked = [moved[back - 1] * masks[back - 1] for back in range(1, TAPS)]
    for back in range(1, TAPS):
        total = total + masked[back - 1] * taps_ref[TAPS - 1 - back : TAPS - back, lanes]
    return total, masked


def order_masks():
    row = lax.broadcasted_iota(jnp.int32, (CHUNK, CHUNK), 0)
    column = lax.broadcasted_iota(jnp.int32, (CHUNK, CHUNK), 1)
    return row, column


def rates(sraw_ref, heads_ref):
    lane = lax.broadcasted_iota(jnp.int32, (CHUNK, LANES), 1)
    raw = sraw_ref[...] + heads_ref[0:1, :]
    step = jnp.where(lane < HEADS, softplus(raw), 0.0)
    rate = step * heads_ref[1:2, :]
    row, column = order_masks()
    lower = (row >= column).astype(F32)
    cumulative = exact_dot(lower, rate)
    return raw, step, rate, cumulative


def factors(cumulative, cols_ref):
    lane = lax.broadcasted_iota(jnp.int32, (CHUNK, LANES), 1)
    keep = lane < HEADS
    last = cumulative[CHUNK - 1 : CHUNK, :]
    stay = jnp.where(keep, jnp.exp(last - cumulative) * cols_ref[:, 4:5], 0.0)
    come = jnp.where(keep, jnp.exp(cumulative) * cols_ref[:, 3:4], 0.0)
    return stay, come


def pair_of(block):
    lane = lax.broadcasted_iota(jnp.int32, block.shape, 1)
    zero = jnp.zeros_like(block)
    return jnp.concatenate(
        [jnp.where(lane < HEAD_DIM, block, zero), jnp.where(lane >= HEAD_DIM, block, zero)], axis=0
    )


def scan_forward(
    x_ref,
    tail_ref,
    sraw_ref,
    cols_ref,
    segrow_ref,
    taps_ref,
    heads_ref,
    spread_ref,
    core_ref,
    conv_ref,
    maps_ref,
    reach_ref,
    state_ref,
    decay_ref,
    carry,
    run,
):
    chunk = pl.program_id(1)

    @pl.when(chunk == 0)
    def _():
        carry[...] = jnp.zeros_like(carry)
        run[...] = jnp.zeros_like(run)

    masks = [wide(cols_ref[:, k : k + 1]) for k in range(TAPS - 1)]
    _, step, rate, cumulative = rates(sraw_ref, heads_ref)
    stay, come = factors(cumulative, cols_ref)
    lane = lax.broadcasted_iota(jnp.int32, (CHUNK, LANES), 1)
    whole = cumulative + run[0:1, :]
    reach = jnp.where(lane < HEADS, jnp.exp(whole) * cols_ref[:, 7:8], 0.0)
    reach_ref[...] = reach
    run[...] = jnp.broadcast_to(whole[CHUNK - 1 : CHUNK, :], run.shape)
    decay_ref[0, 0] = nn(doubled(jnp.broadcast_to(reach[CHUNK - 1 : CHUNK, :], (16, LANES))), spread_ref[...])[:8]

    maps = []
    for part in range(2):
        lanes = slice(INNER + part * STATE, INNER + (part + 1) * STATE)
        block = x_ref[:, lanes].astype(F32)
        total, _ = total_of(block, shifted(block, tail_ref[0, :, lanes].astype(F32)), masks, taps_ref, lanes)
        maps.append((total * sigmoid(total)).astype(BF))
        maps_ref[:, part * STATE : (part + 1) * STATE] = maps[part]
    entry, reader = maps
    row, column = order_masks()
    same = (row >= column) & (wide(cols_ref[:, 5:6]) == segrow_ref[0, 0:1, :])
    inner = jnp.where(same, nt(reader, entry), 0.0)
    entry_t = jnp.transpose(entry.astype(F32)).astype(BF)
    cum_t = jnp.transpose(cumulative)
    step2, stay2, come2 = doubled(step), doubled(stay), doubled(come)

    for group in range(INNER // GROUP):
        span = slice(group * GROUP, (group + 1) * GROUP)
        step_x = nn(step2, spread_ref[:, span])
        stay_x = nn(stay2, spread_ref[:, span])
        come_x = nn(come2, spread_ref[:, span])
        old = carry[:, span]
        brought = nn(reader, old.astype(BF)) * come_x
        kept = []
        for half in range(GROUP // LANES):
            lanes = slice(group * GROUP + half * LANES, group * GROUP + (half + 1) * LANES)
            local = slice(half * LANES, (half + 1) * LANES)
            block = x_ref[:, lanes].astype(F32)
            total, _ = total_of(block, shifted(block, tail_ref[0, :, lanes].astype(F32)), masks, taps_ref, lanes)
            convolved = total * sigmoid(total)
            conv_ref[:, lanes] = convolved.astype(BF)
            scaled = (convolved * step_x[:, local]).astype(BF)
            kept.append((scaled.astype(F32) * stay_x[:, local]).astype(BF))
            weights = []
            for head in (group * 4 + half * 2, group * 4 + half * 2 + 1):
                gap = wide(cumulative[:, head : head + 1]) - cum_t[head : head + 1, :]
                weights.append((inner * jnp.exp(jnp.minimum(gap, 0.0))).astype(BF))
            diagonal = nn(jnp.concatenate(weights, axis=1), pair_of(scaled))
            core_ref[:, lanes] = diagonal + brought[:, local]
        fresh = nn(entry_t, jnp.concatenate(kept, axis=1))
        fresh = old * come_x[CHUNK - 1 : CHUNK, :] + fresh
        carry[:, span] = fresh
        state_ref[0, 0, :, span] = fresh.astype(BF)


def scan_backward(
    x_ref,
    tail_ref,
    sraw_ref,
    cols_ref,
    segrow_ref,
    taps_ref,
    heads_ref,
    spread_ref,
    gather_ref,
    out_ref,
    rows_ref,
    state_ref,
    decay_ref,
    enter_ref,
    back_ref,
    grad_ref,
    raw_ref,
    halo_ref,
    acc_ref,
    head_acc_ref,
    carry,
    later,
):
    micro = pl.program_id(0)
    chunk = pl.num_programs(1) - 1 - pl.program_id(1)

    @pl.when((micro == 0) & (pl.program_id(1) == 0))
    def _():
        acc_ref[...] = jnp.zeros_like(acc_ref)
        head_acc_ref[...] = jnp.zeros_like(head_acc_ref)

    first = pl.program_id(1) == 0
    start = chunk == 0
    gather = gather_ref[...]

    @pl.when(first)
    def _():
        later[...] = jnp.zeros_like(later)
        carry[...] = back_ref[0].astype(F32)

    masks = [wide(cols_ref[:, k : k + 1]) for k in range(TAPS - 1)]
    raw, step, rate, cumulative = rates(sraw_ref, heads_ref)
    stay, come = factors(cumulative, cols_ref)

    maps = []
    for part in range(2):
        lanes = slice(INNER + part * STATE, INNER + (part + 1) * STATE)
        block = x_ref[:, lanes].astype(F32)
        moved = shifted(block, tail_ref[0, :, lanes].astype(F32))
        total, masked = total_of(block, moved, masks, taps_ref, lanes)
        gate = sigmoid(total)
        maps.append(((total * gate).astype(BF), gate * (1.0 + total * (1.0 - gate)), block, masked))
    entry, reader = maps[0][0], maps[1][0]
    row, column = order_masks()
    same = (row >= column) & (wide(cols_ref[:, 5:6]) == segrow_ref[0, 0:1, :])
    inner = jnp.where(same, nt(reader, entry), 0.0)
    reader_t = jnp.transpose(reader.astype(F32)).astype(BF)
    cum_t = jnp.transpose(cumulative)
    step2, stay2, come2 = doubled(step), doubled(stay), doubled(come)

    back_inner = jnp.zeros((CHUNK, CHUNK), F32)
    back_entry = jnp.zeros((CHUNK, STATE), F32)
    back_reader = jnp.zeros((CHUNK, STATE), F32)
    columns = jnp.zeros((CHUNK, LANES), F32)
    steps = jnp.zeros((CHUNK, LANES), F32)
    products = []

    def conv_back(back_total, block, masked, lanes):
        parts = [back_total * block] + [back_total * value for value in masked]
        for index, value in enumerate([back_total] + parts):
            acc_ref[index * 8 : index * 8 + 8, lanes] += jnp.sum(value.reshape(CHUNK // 8, 8, LANES), axis=0)
        result = back_total * taps_ref[TAPS - 1 : TAPS, lanes]
        edge = jnp.zeros((8, LANES), F32)
        for back in range(1, TAPS):
            held = back_total * masks[back - 1]
            full = jnp.concatenate([held, later[back - 1, :, lanes]], axis=0)
            tap = taps_ref[TAPS - 1 - back : TAPS - back, lanes]
            result = result + pltpu.roll(full, CHUNK + 8 - back, 0)[:CHUNK] * tap
            head = jnp.concatenate([jnp.zeros((8, LANES), F32), held[:8]], axis=0)
            edge = edge + pltpu.roll(head, 16 - back, 0)[:8] * tap
            later[back - 1, :, lanes] = held[:8]
        grad_ref[:, lanes] = result.astype(BF)
        halo_ref[0, :, lanes] = edge.astype(BF)

    for group in range(INNER // GROUP):
        span = slice(group * GROUP, (group + 1) * GROUP)
        step_x = nn(step2, spread_ref[:, span])
        stay_x = nn(stay2, spread_ref[:, span])
        come_x = nn(come2, spread_ref[:, span])
        back_carry = carry[:, span]
        back_low = back_carry.astype(BF)
        from_state = nn(entry, back_low) * stay_x
        out = out_ref[:, span]
        out_f = out.astype(F32)
        come_out = (out_f * come_x).astype(BF)
        enter = enter_ref[0, :, span].astype(F32)
        before = jnp.where(
            start, enter, state_ref[0, 0, :, span].astype(F32) + enter * decay_ref[0, 0, 0:1, span]
        )
        back_reader = back_reader + nt(come_out, before.astype(BF))
        kept = []
        within = []
        for half in range(GROUP // LANES):
            lanes = slice(group * GROUP + half * LANES, group * GROUP + (half + 1) * LANES)
            local = slice(half * LANES, (half + 1) * LANES)
            block = x_ref[:, lanes].astype(F32)
            moved = shifted(block, tail_ref[0, :, lanes].astype(F32))
            total, masked = total_of(block, moved, masks, taps_ref, lanes)
            gate = sigmoid(total)
            convolved = total * gate
            slope = gate * (1.0 + total * (1.0 - gate))
            scaled = (convolved * step_x[:, local]).astype(BF)
            scaled_f = scaled.astype(F32)
            kept.append((scaled_f * stay_x[:, local]).astype(BF))
            within.append(jnp.sum(scaled_f * from_state[:, local], axis=0, keepdims=True))
            back_pair = nt(out[:, local], pair_of(scaled))
            weights = []
            for index in range(2):
                head = group * 4 + half * 2 + index
                gap = wide(cumulative[:, head : head + 1]) - cum_t[head : head + 1, :]
                table = jnp.exp(jnp.minimum(gap, 0.0))
                weights.append((inner * table).astype(BF))
                back_inner = back_inner + back_pair[:, index * CHUNK : (index + 1) * CHUNK] * table
            back_scaled = tn(jnp.concatenate(weights, axis=0), pair_of(out[:, local])) + from_state[:, local]
            high, low = pieces(scaled_f * back_scaled)
            columns = columns + nn(high, gather[lanes, :]) + nn(low, gather[lanes, :])
            steps = steps + nn((convolved * back_scaled).astype(BF), gather[lanes, :])
            back_convolved = out_f[:, local] * taps_ref[5:6, lanes] + back_scaled * step_x[:, local]
            conv_back(back_convolved * slope, block, masked, lanes)
        back_entry = back_entry + nt(jnp.concatenate(kept, axis=1), back_low)
        decayed = back_carry * come_x[CHUNK - 1 : CHUNK, :]
        carry[:, span] = decayed + nn(reader_t, come_out)
        products.append(jnp.sum(decayed * before, axis=0, keepdims=True) + jnp.concatenate(within, axis=1))

    back_inner = jnp.where(same, back_inner, 0.0).astype(BF)
    back_reader = back_reader + nn(back_inner, entry)
    back_entry = back_entry + tn(back_inner, reader)
    for part, value in ((0, back_entry), (1, back_reader)):
        lanes = slice(INNER + part * STATE, INNER + (part + 1) * STATE)
        conv_back(value * maps[part][1], maps[part][2], maps[part][3], lanes)

    high, low = pieces(jnp.broadcast_to(jnp.concatenate(products, axis=1), (16, INNER)))
    gamma = nn(high, gather) + nn(low, gather)
    ends = jnp.where(row[:, :LANES] == CHUNK - 1, gamma[0:1, :], 0.0)
    back_cumulative = rows_ref[...] - columns + ends
    upper = (row <= column).astype(F32)
    back_rate = exact_dot(upper, back_cumulative)
    back_step = steps + back_rate * heads_ref[1:2, :]
    back_raw = back_step * sigmoid(raw)
    raw_ref[...] = back_raw.astype(BF)
    head_acc_ref[0:8, :] += jnp.sum(back_raw.reshape(CHUNK // 8, 8, LANES), axis=0)
    head_acc_ref[8:16, :] += jnp.sum((back_rate * rate).reshape(CHUNK // 8, 8, LANES), axis=0)


def constant(shape):
    return pl.BlockSpec(shape, lambda m, c: (0,) * len(shape))


def run_forward(x, tails, sraw, cols, segrow, taps, heads, spread, chunks):
    rows = x.shape[0]
    micro = rows // (chunks * CHUNK)
    flat = lambda width: pl.BlockSpec((CHUNK, width), lambda m, c: (m * chunks + c, 0))
    return pl.pallas_call(
        scan_forward,
        grid=(micro, chunks),
        in_specs=[
            flat(CHANNELS),
            pl.BlockSpec((1, 8, CHANNELS), lambda m, c: (m * chunks + c, 0, 0)),
            flat(LANES),
            flat(LANES),
            pl.BlockSpec((1, 8, LANES), lambda m, c: (m * chunks + c, 0, 0)),
            constant((8, CHANNELS)),
            constant((8, LANES)),
            constant((LANES, INNER)),
        ],
        out_specs=[
            flat(INNER),
            flat(INNER),
            flat(2 * STATE),
            flat(LANES),
            pl.BlockSpec((1, 1, STATE, INNER), lambda m, c: (m, c, 0, 0)),
            pl.BlockSpec((1, 1, 8, INNER), lambda m, c: (m, c, 0, 0)),
        ],
        out_shape=[
            jax.ShapeDtypeStruct((rows, INNER), F32),
            jax.ShapeDtypeStruct((rows, INNER), BF),
            jax.ShapeDtypeStruct((rows, 2 * STATE), BF),
            jax.ShapeDtypeStruct((rows, LANES), F32),
            jax.ShapeDtypeStruct((micro, chunks, STATE, INNER), BF),
            jax.ShapeDtypeStruct((micro, chunks, 8, INNER), F32),
        ],
        scratch_shapes=[pltpu.VMEM((STATE, INNER), F32), pltpu.VMEM((8, LANES), F32)],
        compiler_params=pltpu.CompilerParams(vmem_limit_bytes=VMEM_LIMIT),
        name="scan_forward",
    )(x, tails, sraw, cols, segrow, taps, heads, spread)


def run_backward(x, tails, sraw, cols, segrow, taps, heads, spread, gather, out, row_sums, states, decay, enter, back, chunks):
    rows = x.shape[0]
    micro = rows // (chunks * CHUNK)
    place = lambda m, c: m * chunks + chunks - 1 - c
    flat = lambda width: pl.BlockSpec((CHUNK, width), lambda m, c: (place(m, c), 0))
    return pl.pallas_call(
        scan_backward,
        grid=(micro, chunks),
        in_specs=[
            flat(CHANNELS),
            pl.BlockSpec((1, 8, CHANNELS), lambda m, c: (place(m, c), 0, 0)),
            flat(LANES),
            flat(LANES),
            pl.BlockSpec((1, 8, LANES), lambda m, c: (place(m, c), 0, 0)),
            constant((8, CHANNELS)),
            constant((8, LANES)),
            constant((LANES, INNER)),
            constant((INNER, LANES)),
            flat(INNER),
            flat(LANES),
            pl.BlockSpec((1, 1, STATE, INNER), lambda m, c: (m, jnp.maximum(chunks - 2 - c, 0), 0, 0)),
            pl.BlockSpec((1, 1, 8, INNER), lambda m, c: (m, jnp.maximum(chunks - 2 - c, 0), 0, 0)),
            pl.BlockSpec((1, STATE, INNER), lambda m, c: (m, 0, 0)),
            pl.BlockSpec((1, STATE, INNER), lambda m, c: (m, 0, 0)),
        ],
        out_specs=[
            flat(CHANNELS),
            flat(LANES),
            pl.BlockSpec((1, 8, CHANNELS), lambda m, c: (m, 0, 0)),
            constant((40, CHANNELS)),
            constant((16, LANES)),
        ],
        out_shape=[
            jax.ShapeDtypeStruct((rows, CHANNELS), BF),
            jax.ShapeDtypeStruct((rows, LANES), BF),
            jax.ShapeDtypeStruct((micro, 8, CHANNELS), BF),
            jax.ShapeDtypeStruct((40, CHANNELS), F32),
            jax.ShapeDtypeStruct((16, LANES), F32),
        ],
        scratch_shapes=[
            pltpu.VMEM((STATE, INNER), F32),
            pltpu.VMEM((TAPS - 1, 8, CHANNELS), F32),
        ],
        compiler_params=pltpu.CompilerParams(vmem_limit_bytes=VMEM_LIMIT),
        name="scan_backward",
    )(x, tails, sraw, cols, segrow, taps, heads, spread, gather, out, row_sums, states, decay, enter, back)


def gather_weights(shards):
    flat = jnp.concatenate([shard.reshape(-1) for shard in shards])
    everyone = lax.all_gather(flat, ("dp", "tensor"), axis=0, tiled=False)
    everyone = everyone.reshape(lax.axis_size("dp"), lax.axis_size("tensor"), flat.shape[0])
    result = []
    start = 0
    for shard in shards:
        result.append(everyone[:, :, start : start + shard.size].reshape(everyone.shape[:2] + shard.shape))
        start += shard.size
    return result


def join(shards, dp_dim, tensor_dim):
    groups, members = shards.shape[:2]
    shape = list(shards.shape[2:])
    order = []
    for dim in range(len(shape)):
        if dim == dp_dim:
            order.append(0)
        if dim == tensor_dim:
            order.append(1)
        order.append(dim + 2)
    full = shape[:]
    full[dp_dim] *= groups
    full[tensor_dim] *= members
    return jnp.transpose(shards, order).reshape(full)


def cut(full, dp_dim, tensor_dim):
    groups, members = lax.axis_size("dp"), lax.axis_size("tensor")
    shape = []
    for dim, size in enumerate(full.shape):
        if dim == dp_dim:
            shape.append(groups)
            size //= groups
        if dim == tensor_dim:
            shape.append(members)
            size //= members
        shape.append(size)
    both = full.reshape(shape)
    position = dp_dim + (1 if tensor_dim < dp_dim else 0)
    where = tensor_dim + (1 if dp_dim <= tensor_dim else 0)
    return jnp.moveaxis(both, (position, where), (0, 1))


def reduce_shards(grads, places, shapes):
    groups, members = lax.axis_size("dp"), lax.axis_size("tensor")
    flat = jnp.concatenate(
        [cut(grad.astype(BF), *place).reshape(groups * members, -1) for grad, place in zip(grads, places)], axis=1
    )
    mine = lax.psum_scatter(flat, ("dp", "tensor"), scatter_dimension=0, tiled=True).reshape(-1).astype(F32)
    result = []
    start = 0
    for shape in shapes:
        size = 1
        for extent in shape:
            size *= extent
        result.append(mine[start : start + size].reshape(shape))
        start += size
    return result


def chain(own, decay, forward):
    members = lax.axis_size("tensor")
    if forward:
        hops = [(index, index + 1) for index in range(members - 1)]
    else:
        hops = [(index + 1, index) for index in range(members - 1)]
    held = None
    for _ in range(members - 1):
        value = own if held is None else own + decay * held.astype(F32)
        held = lax.ppermute(value.astype(BF), "tensor", hops)
    return held


def marks(bounds, rows, chunks):
    place = lax.axis_index("tensor")
    local = jnp.arange(rows, dtype=jnp.int32)[None, :]
    position = local + place * rows
    first = bounds[:, 0, 0:1]
    used = bounds[:, 0, 1:2]

    def segment_at(where):
        value = (where >= first).astype(jnp.int32) + (where >= used).astype(jnp.int32)
        return jnp.where(where < 0, -1, value)

    segment = segment_at(position)
    start = position - local % CHUNK
    columns = [segment == segment_at(position - back) for back in range(1, TAPS)]
    columns.append(segment == segment_at(start - 1))
    columns.append(segment == segment_at(start + CHUNK - 1))
    columns.append(segment)
    columns.append(position < used)
    columns.append(segment == segment_at(position * 0 + place * rows - 1))
    lane = lax.broadcasted_iota(jnp.int32, (1, 1, LANES), 2)
    table = jnp.zeros(segment.shape + (LANES,), F32)
    for index, column in enumerate(columns):
        table = jnp.where(lane == index, column.astype(F32)[:, :, None], table)
    across = jnp.broadcast_to(
        segment.astype(F32).reshape(-1, 1, CHUNK), (segment.shape[0] * chunks, 8, CHUNK)
    )
    return table.reshape(-1, LANES), across


def local(
    stream,
    bounds,
    prescale,
    expansion,
    timestep,
    selection,
    kernels,
    biases,
    stencil,
    baseline,
    offset,
    decays,
    passthrough,
    rescale,
    readout,
    cotangent,
):
    members = lax.axis_size("tensor")
    place = lax.axis_index("tensor")
    micro, rows = stream.shape[:2]
    chunks = rows // CHUNK
    assert rows * members == SLOT and bounds.shape[1] == 1
    weights = (prescale, expansion, timestep, selection, kernels, biases, stencil, baseline, offset, decays, passthrough, rescale, readout)
    got = gather_weights(weights)
    prescale_full = got[0].reshape(WIDTH).astype(F32)
    expand = join(got[1], 0, 2)
    time_full = join(got[2], 0, 1)
    select = got[3].reshape(WIDTH, 2 * STATE)
    kernel_full = join(got[4], 1, 0).reshape(INNER, TAPS)
    bias_full = join(got[5], 1, 0).reshape(INNER)
    stencil_full = got[6].reshape(2 * STATE, TAPS)
    baseline_full = got[7].reshape(2 * STATE)
    offset_full, decays_full, pass_full = (item[0].reshape(HEADS).astype(F32) for item in got[8:11])
    rescale_full = join(got[11], 1, 0).reshape(1, INNER).astype(F32)
    readout_full = join(got[12], 1, 0)

    head = lax.broadcasted_iota(jnp.int32, (LANES, INNER), 0)
    channel = lax.broadcasted_iota(jnp.int32, (LANES, INNER), 1) // HEAD_DIM
    spread = ((head < 2 * HEADS) & (head % HEADS == channel)).astype(BF)
    gather = ((head < HEADS) & (head == channel)).astype(BF).T
    pass_wide = jnp.repeat(pass_full, HEAD_DIM)
    taps = jnp.concatenate([kernel_full, stencil_full], axis=0).astype(F32).T
    shifts = jnp.concatenate([bias_full, baseline_full]).astype(F32)[None]
    last = jnp.concatenate([pass_wide, jnp.zeros((2 * STATE,), F32)])[None]
    taps = jnp.concatenate([taps, shifts, last, jnp.zeros((2, CHANNELS), F32)], axis=0)
    heads = jnp.pad(jnp.stack([offset_full, -jnp.exp(decays_full)]), ((0, 6), (0, LANES - HEADS)))
    cols, segrow = marks(bounds, rows, chunks)

    flat = stream.reshape(micro * rows, WIDTH)

    def low_norm(values):
        values = values.astype(F32)
        return (values * lax.rsqrt(jnp.mean(values * values, axis=-1, keepdims=True) + EPS) * prescale_full).astype(BF)

    hops = [(index, index + 1) for index in range(members - 1)]
    edge = lax.ppermute(stream[:, rows - 8 :, :], "tensor", hops).reshape(micro * 8, WIDTH)
    lowered = low_norm(flat)
    lowered_edge = low_norm(edge)
    signal_weight = jnp.concatenate([expand[:, 1, :], select], axis=1)
    gate_weight = expand[:, 0, :]
    time_weight = jnp.pad(time_full, ((0, 0), (0, LANES - HEADS)))
    signal = nn(lowered, signal_weight).astype(BF)
    signal_edge = nn(lowered_edge, signal_weight).astype(BF)
    gate = nn(lowered, gate_weight).astype(BF)
    sraw = nn(lowered, time_weight)
    tails = jnp.concatenate(
        [
            signal_edge.reshape(micro, 1, 8, CHANNELS),
            signal.reshape(micro, chunks, CHUNK, CHANNELS)[:, : chunks - 1, CHUNK - 8 :, :],
        ],
        axis=1,
    ).reshape(micro * chunks, 8, CHANNELS)
    core, convolved, maps, reach, states, decay = run_forward(
        signal, tails, sraw, cols, segrow, taps, heads, spread, chunks
    )
    total_decay = decay[:, chunks - 1, 0:1, :]
    enter = chain(states[:, chunks - 1].astype(F32), total_decay, True)

    reader = maps[:, STATE:]
    high = reach.astype(BF)
    reach_x = nn(high, gather.T) + nn((reach - high.astype(F32)).astype(BF), gather.T)
    brought = jnp.einsum(
        "min,mnk->mik", reader.reshape(micro, rows, STATE), enter, preferred_element_type=F32
    ).reshape(micro * rows, INNER)
    core = core + brought * reach_x
    conv_f = convolved.astype(F32)
    output = core + pass_wide * conv_f
    gate_f = gate.astype(F32)
    open_gate = jax.nn.sigmoid(gate_f)
    silu = gate_f * open_gate
    gated = output * silu
    inverse = lax.rsqrt(jnp.mean(gated * gated, axis=1, keepdims=True) + EPS)
    lifted = (gated * inverse * rescale_full).astype(BF)
    live = cols[:, 6:7]
    mixer = nn(lifted, readout_full)
    result = (flat.astype(F32) + live * mixer).astype(BF)
    cot = cotangent.reshape(micro * rows, WIDTH)
    back_mixer = jnp.where(live > 0, cot, jnp.zeros_like(cot))
    readout_term = tn(lifted, back_mixer)
    back_lifted = nt(back_mixer, readout_full)
    rescale_term = jnp.sum(back_lifted * gated * inverse, axis=0)
    weighted = back_lifted * rescale_full
    dots = jnp.sum(weighted * gated, axis=1, keepdims=True)
    back_gated = inverse * weighted - gated * (inverse * inverse * inverse) * (dots / INNER)
    out = (back_gated * silu).astype(BF)
    back_gate = (back_gated * output * open_gate * (1.0 + gate_f * (1.0 - open_gate))).astype(BF)
    out_f = out.astype(F32)
    pass_term = jnp.sum(jnp.sum(out_f * conv_f, axis=0).reshape(HEADS, HEAD_DIM), axis=1)
    row_sums = jnp.sum((out_f * core).reshape(micro * rows, HEADS, HEAD_DIM), axis=2)
    row_sums = jnp.pad(row_sums, ((0, 0), (0, LANES - HEADS)))
    back_enter = jnp.einsum(
        "min,mik->mnk",
        reader.reshape(micro, rows, STATE),
        (out_f * reach_x).astype(BF).reshape(micro, rows, INNER),
        preferred_element_type=F32,
    )
    back = chain(back_enter, total_decay, False)

    grad_signal, back_raw, halo, acc, head_acc = run_backward(
        signal, tails, sraw, cols, segrow, taps, heads, spread, gather, out, row_sums, states, decay, enter, back, chunks
    )
    returned = lax.ppermute(halo, "tensor", [(index + 1, index) for index in range(members - 1)])
    grad_signal = grad_signal.reshape(micro, rows, CHANNELS)
    fixed = (grad_signal[:, rows - 8 :].astype(F32) + returned.astype(F32)).astype(BF)
    grad_signal = lax.dynamic_update_slice_in_dim(grad_signal, fixed, rows - 8, 1).reshape(micro * rows, CHANNELS)

    gate_term = tn(lowered, back_gate)
    signal_term = tn(lowered, grad_signal)
    time_term = tn(lowered, back_raw)[:, :HEADS]
    back_lowered = nt(back_gate, gate_weight) + nt(grad_signal, signal_weight) + nt(back_raw, time_weight)
    values = flat.astype(F32)
    scale = lax.rsqrt(jnp.mean(values * values, axis=-1, keepdims=True) + EPS)
    prescale_term = jnp.sum(back_lowered * values * scale, axis=0)
    held = back_lowered * prescale_full
    grad_stream = held * scale - values * (scale * scale * scale) * jnp.mean(held * values, axis=-1, keepdims=True)
    grad_stream = (cot.astype(F32) + grad_stream).astype(BF)

    sums = jnp.sum(acc.reshape(5, 8, CHANNELS), axis=1)
    tap_terms = jnp.stack([sums[4], sums[3], sums[2], sums[1]], axis=1)
    head_sums = jnp.sum(head_acc.reshape(2, 8, LANES), axis=1)[:, :HEADS]
    grads = (
        prescale_term[:, None],
        jnp.stack([gate_term, signal_term[:, :INNER]], axis=1),
        time_term,
        signal_term[:, INNER:],
        tap_terms[:INNER].reshape(HEADS, HEAD_DIM * TAPS),
        sums[0, :INNER].reshape(HEADS, HEAD_DIM),
        tap_terms[INNER:],
        sums[0, INNER:][:, None],
        rescale_term.reshape(HEADS, HEAD_DIM),
        readout_term,
    )
    both = ((0, 0), (0, 2), (0, 1), (0, 0), (1, 0), (1, 0), (0, 0), (0, 0), (1, 0), (1, 0))
    shapes = [item.shape for item in (prescale, expansion, timestep, selection, kernels, biases, stencil, baseline, rescale, readout)]
    done = reduce_shards(grads, both, shapes)
    scalars = lax.psum(jnp.stack([head_sums[0], head_sums[1], pass_term]), ("dp", "tensor"))
    scalars = lax.dynamic_slice_in_dim(scalars, place * offset.shape[0], offset.shape[0], axis=1)
    return (
        result.reshape(stream.shape),
        grad_stream.reshape(stream.shape),
        done[0],
        done[1],
        done[2],
        done[3],
        done[4],
        done[5],
        done[6],
        done[7],
        scalars[0],
        scalars[1],
        scalars[2],
        done[8],
        done[9],
    )


def solution(mesh):
    everything = ("dp", "tensor")
    rows = P(None, everything, None)
    weights = (
        P(everything),
        P("dp", None, "tensor"),
        P("dp", "tensor"),
        P(everything, None),
        P("tensor", "dp"),
        P("tensor", "dp"),
        P(everything, None),
        P(everything),
        P("tensor"),
        P("tensor"),
        P("tensor"),
        P("tensor", "dp"),
        P("tensor", "dp"),
    )
    return jax.shard_map(
        local,
        mesh=mesh,
        in_specs=(rows, P(None, "dp", None)) + weights + (rows,),
        out_specs=(rows, rows) + weights,
        check_vma=False,
    )
```

```python
import functools

import jax
import jax.numpy as jnp
from jax import lax
from jax.experimental import pallas as pl
from jax.experimental.pallas import tpu as pltpu
from jax.sharding import PartitionSpec as P

WIDTH = 768
HEADS = 24
HEAD_DIM = 64
STATE = 128
TAPS = 4
INNER = 1536
SLOT = 1024
CHUNK = 128
LANES = 128
GROUP = 256
CHANNELS = INNER + 2 * STATE
EPS = 1e-05
BF = jnp.bfloat16
F32 = jnp.float32
VMEM_LIMIT = 56 * 1024 * 1024


def nn(a, b):
    return lax.dot_general(a, b, (((1,), (0,)), ((), ())), preferred_element_type=F32)


def nt(a, b):
    return lax.dot_general(a, b, (((1,), (1,)), ((), ())), preferred_element_type=F32)


def tn(a, b):
    return lax.dot_general(a, b, (((0,), (0,)), ((), ())), preferred_element_type=F32)


def exact_dot(a, b):
    return lax.dot_general(
        a, b, (((1,), (0,)), ((), ())), preferred_element_type=F32, precision=lax.Precision.HIGHEST
    )


def pieces(v):
    high = v.astype(BF)
    low = (v - high.astype(F32)).astype(BF)
    return high, low


def doubled(v):
    high, low = pieces(v)
    return (high.astype(F32) + pltpu.roll(low.astype(F32), HEADS, 1)).astype(BF)


def softplus(v):
    return jnp.maximum(v, 0.0) + jnp.log1p(jnp.exp(-jnp.abs(v)))


def sigmoid(v):
    return 1.0 / (1.0 + jnp.exp(-v))


def wide(column):
    return jnp.broadcast_to(column, (CHUNK, LANES))


def shifted(block, tail):
    full = jnp.concatenate([tail, block], axis=0)
    return [pltpu.roll(full, back, 0)[8:] for back in range(1, TAPS)]


def total_of(block, moved, masks, taps_ref, lanes):
    total = taps_ref[TAPS : TAPS + 1, lanes] + block * taps_ref[TAPS - 1 : TAPS, lanes]
    masked = [moved[back - 1] * masks[back - 1] for back in range(1, TAPS)]
    for back in range(1, TAPS):
        total = total + masked[back - 1] * taps_ref[TAPS - 1 - back : TAPS - back, lanes]
    return total, masked


def order_masks():
    row = lax.broadcasted_iota(jnp.int32, (CHUNK, CHUNK), 0)
    column = lax.broadcasted_iota(jnp.int32, (CHUNK, CHUNK), 1)
    return row, column


def rates(sraw_ref, heads_ref):
    lane = lax.broadcasted_iota(jnp.int32, (CHUNK, LANES), 1)
    raw = sraw_ref[...] + heads_ref[0:1, :]
    step = jnp.where(lane < HEADS, softplus(raw), 0.0)
    rate = step * heads_ref[1:2, :]
    row, column = order_masks()
    lower = (row >= column).astype(F32)
    cumulative = exact_dot(lower, rate)
    return raw, step, rate, cumulative


def factors(cumulative, cols_ref):
    lane = lax.broadcasted_iota(jnp.int32, (CHUNK, LANES), 1)
    keep = lane < HEADS
    last = cumulative[CHUNK - 1 : CHUNK, :]
    stay = jnp.where(keep, jnp.exp(last - cumulative) * cols_ref[:, 4:5], 0.0)
    come = jnp.where(keep, jnp.exp(cumulative) * cols_ref[:, 3:4], 0.0)
    return stay, come


def pair_of(block):
    lane = lax.broadcasted_iota(jnp.int32, block.shape, 1)
    zero = jnp.zeros_like(block)
    return jnp.concatenate(
        [jnp.where(lane < HEAD_DIM, block, zero), jnp.where(lane >= HEAD_DIM, block, zero)], axis=0
    )


def scan_forward(
    x_ref,
    tail_ref,
    sraw_ref,
    cols_ref,
    segrow_ref,
    taps_ref,
    heads_ref,
    spread_ref,
    core_ref,
    conv_ref,
    maps_ref,
    reach_ref,
    state_ref,
    decay_ref,
    carry,
    run,
):
    chunk = pl.program_id(1)

    @pl.when(chunk == 0)
    def _():
        carry[...] = jnp.zeros_like(carry)
        run[...] = jnp.zeros_like(run)

    masks = [wide(cols_ref[:, k : k + 1]) for k in range(TAPS - 1)]
    _, step, rate, cumulative = rates(sraw_ref, heads_ref)
    stay, come = factors(cumulative, cols_ref)
    lane = lax.broadcasted_iota(jnp.int32, (CHUNK, LANES), 1)
    whole = cumulative + run[0:1, :]
    reach = jnp.where(lane < HEADS, jnp.exp(whole) * cols_ref[:, 7:8], 0.0)
    reach_ref[...] = reach
    run[...] = jnp.broadcast_to(whole[CHUNK - 1 : CHUNK, :], run.shape)
    decay_ref[0, 0] = nn(doubled(jnp.broadcast_to(reach[CHUNK - 1 : CHUNK, :], (16, LANES))), spread_ref[...])[:8]

    maps = []
    for part in range(2):
        lanes = slice(INNER + part * STATE, INNER + (part + 1) * STATE)
        block = x_ref[:, lanes].astype(F32)
        total, _ = total_of(block, shifted(block, tail_ref[0, :, lanes].astype(F32)), masks, taps_ref, lanes)
        maps.append((total * sigmoid(total)).astype(BF))
        maps_ref[:, part * STATE : (part + 1) * STATE] = maps[part]
    entry, reader = maps
    row, column = order_masks()
    same = (row >= column) & (wide(cols_ref[:, 5:6]) == segrow_ref[0, 0:1, :])
    inner = jnp.where(same, nt(reader, entry), 0.0)
    entry_t = jnp.transpose(entry.astype(F32)).astype(BF)
    cum_t = jnp.transpose(cumulative)
    step2, stay2, come2 = doubled(step), doubled(stay), doubled(come)

    for group in range(INNER // GROUP):
        span = slice(group * GROUP, (group + 1) * GROUP)
        step_x = nn(step2, spread_ref[:, span])
        stay_x = nn(stay2, spread_ref[:, span])
        come_x = nn(come2, spread_ref[:, span])
        old = carry[:, span]
        brought = nn(reader, old.astype(BF)) * come_x
        kept = []
        for half in range(GROUP // LANES):
            lanes = slice(group * GROUP + half * LANES, group * GROUP + (half + 1) * LANES)
            local = slice(half * LANES, (half + 1) * LANES)
            block = x_ref[:, lanes].astype(F32)
            total, _ = total_of(block, shifted(block, tail_ref[0, :, lanes].astype(F32)), masks, taps_ref, lanes)
            convolved = total * sigmoid(total)
            conv_ref[:, lanes] = convolved.astype(BF)
            scaled = (convolved * step_x[:, local]).astype(BF)
            kept.append((scaled.astype(F32) * stay_x[:, local]).astype(BF))
            weights = []
            for head in (group * 4 + half * 2, group * 4 + half * 2 + 1):
                gap = wide(cumulative[:, head : head + 1]) - cum_t[head : head + 1, :]
                weights.append((inner * jnp.exp(jnp.minimum(gap, 0.0))).astype(BF))
            diagonal = nn(jnp.concatenate(weights, axis=1), pair_of(scaled))
            core_ref[:, lanes] = diagonal + brought[:, local]
        fresh = nn(entry_t, jnp.concatenate(kept, axis=1))
        fresh = old * come_x[CHUNK - 1 : CHUNK, :] + fresh
        carry[:, span] = fresh
        state_ref[0, 0, :, span] = fresh.astype(BF)


def scan_backward(
    x_ref,
    tail_ref,
    sraw_ref,
    cols_ref,
    segrow_ref,
    taps_ref,
    heads_ref,
    spread_ref,
    gather_ref,
    out_ref,
    rows_ref,
    state_ref,
    decay_ref,
    enter_ref,
    back_ref,
    grad_ref,
    raw_ref,
    halo_ref,
    acc_ref,
    head_acc_ref,
    carry,
    later,
):
    micro = pl.program_id(0)
    chunk = pl.num_programs(1) - 1 - pl.program_id(1)

    @pl.when((micro == 0) & (pl.program_id(1) == 0))
    def _():
        acc_ref[...] = jnp.zeros_like(acc_ref)
        head_acc_ref[...] = jnp.zeros_like(head_acc_ref)

    first = pl.program_id(1) == 0
    start = chunk == 0
    gather = gather_ref[...]

    @pl.when(first)
    def _():
        later[...] = jnp.zeros_like(later)
        carry[...] = back_ref[0].astype(F32)

    masks = [wide(cols_ref[:, k : k + 1]) for k in range(TAPS - 1)]
    raw, step, rate, cumulative = rates(sraw_ref, heads_ref)
    stay, come = factors(cumulative, cols_ref)

    maps = []
    for part in range(2):
        lanes = slice(INNER + part * STATE, INNER + (part + 1) * STATE)
        block = x_ref[:, lanes].astype(F32)
        moved = shifted(block, tail_ref[0, :, lanes].astype(F32))
        total, masked = total_of(block, moved, masks, taps_ref, lanes)
        gate = sigmoid(total)
        maps.append(((total * gate).astype(BF), gate * (1.0 + total * (1.0 - gate)), block, masked))
    entry, reader = maps[0][0], maps[1][0]
    row, column = order_masks()
    same = (row >= column) & (wide(cols_ref[:, 5:6]) == segrow_ref[0, 0:1, :])
    inner = jnp.where(same, nt(reader, entry), 0.0)
    reader_t = jnp.transpose(reader.astype(F32)).astype(BF)
    cum_t = jnp.transpose(cumulative)
    step2, stay2, come2 = doubled(step), doubled(stay), doubled(come)

    back_inner = jnp.zeros((CHUNK, CHUNK), F32)
    back_entry = jnp.zeros((CHUNK, STATE), F32)
    back_reader = jnp.zeros((CHUNK, STATE), F32)
    columns = jnp.zeros((CHUNK, LANES), F32)
    steps = jnp.zeros((CHUNK, LANES), F32)
    products = []

    def conv_back(back_total, block, masked, lanes):
        parts = [back_total * block] + [back_total * value for value in masked]
        for index, value in enumerate([back_total] + parts):
            acc_ref[index * 8 : index * 8 + 8, lanes] += jnp.sum(value.reshape(CHUNK // 8, 8, LANES), axis=0)
        result = back_total * taps_ref[TAPS - 1 : TAPS, lanes]
        edge = jnp.zeros((8, LANES), F32)
        for back in range(1, TAPS):
            held = back_total * masks[back - 1]
            full = jnp.concatenate([held, later[back - 1, :, lanes]], axis=0)
            tap = taps_ref[TAPS - 1 - back : TAPS - back, lanes]
            result = result + pltpu.roll(full, CHUNK + 8 - back, 0)[:CHUNK] * tap
            head = jnp.concatenate([jnp.zeros((8, LANES), F32), held[:8]], axis=0)
            edge = edge + pltpu.roll(head, 16 - back, 0)[:8] * tap
            later[back - 1, :, lanes] = held[:8]
        grad_ref[:, lanes] = result.astype(BF)
        halo_ref[0, :, lanes] = edge.astype(BF)

    for group in range(INNER // GROUP):
        span = slice(group * GROUP, (group + 1) * GROUP)
        step_x = nn(step2, spread_ref[:, span])
        stay_x = nn(stay2, spread_ref[:, span])
        come_x = nn(come2, spread_ref[:, span])
        back_carry = carry[:, span]
        back_low = back_carry.astype(BF)
        from_state = nn(entry, back_low) * stay_x
        out = out_ref[:, span]
        out_f = out.astype(F32)
        come_out = (out_f * come_x).astype(BF)
        enter = enter_ref[0, :, span].astype(F32)
        before = jnp.where(
            start, enter, state_ref[0, 0, :, span].astype(F32) + enter * decay_ref[0, 0, 0:1, span]
        )
        back_reader = back_reader + nt(come_out, before.astype(BF))
        kept = []
        within = []
        for half in range(GROUP // LANES):
            lanes = slice(group * GROUP + half * LANES, group * GROUP + (half + 1) * LANES)
            local = slice(half * LANES, (half + 1) * LANES)
            block = x_ref[:, lanes].astype(F32)
            moved = shifted(block, tail_ref[0, :, lanes].astype(F32))
            total, masked = total_of(block, moved, masks, taps_ref, lanes)
            gate = sigmoid(total)
            convolved = total * gate
            slope = gate * (1.0 + total * (1.0 - gate))
            scaled = (convolved * step_x[:, local]).astype(BF)
            scaled_f = scaled.astype(F32)
            kept.append((scaled_f * stay_x[:, local]).astype(BF))
            within.append(jnp.sum(scaled_f * from_state[:, local], axis=0, keepdims=True))
            back_pair = nt(out[:, local], pair_of(scaled))
            weights = []
            for index in range(2):
                head = group * 4 + half * 2 + index
                gap = wide(cumulative[:, head : head + 1]) - cum_t[head : head + 1, :]
                table = jnp.exp(jnp.minimum(gap, 0.0))
                weights.append((inner * table).astype(BF))
                back_inner = back_inner + back_pair[:, index * CHUNK : (index + 1) * CHUNK] * table
            back_scaled = tn(jnp.concatenate(weights, axis=0), pair_of(out[:, local])) + from_state[:, local]
            high, low = pieces(scaled_f * back_scaled)
            columns = columns + nn(high, gather[lanes, :]) + nn(low, gather[lanes, :])
            steps = steps + nn((convolved * back_scaled).astype(BF), gather[lanes, :])
            back_convolved = out_f[:, local] * taps_ref[5:6, lanes] + back_scaled * step_x[:, local]
            conv_back(back_convolved * slope, block, masked, lanes)
        back_entry = back_entry + nt(jnp.concatenate(kept, axis=1), back_low)
        decayed = back_carry * come_x[CHUNK - 1 : CHUNK, :]
        carry[:, span] = decayed + nn(reader_t, come_out)
        products.append(jnp.sum(decayed * before, axis=0, keepdims=True) + jnp.concatenate(within, axis=1))

    back_inner = jnp.where(same, back_inner, 0.0).astype(BF)
    back_reader = back_reader + nn(back_inner, entry)
    back_entry = back_entry + tn(back_inner, reader)
    for part, value in ((0, back_entry), (1, back_reader)):
        lanes = slice(INNER + part * STATE, INNER + (part + 1) * STATE)
        conv_back(value * maps[part][1], maps[part][2], maps[part][3], lanes)

    high, low = pieces(jnp.broadcast_to(jnp.concatenate(products, axis=1), (16, INNER)))
    gamma = nn(high, gather) + nn(low, gather)
    ends = jnp.where(row[:, :LANES] == CHUNK - 1, gamma[0:1, :], 0.0)
    back_cumulative = rows_ref[...] - columns + ends
    upper = (row <= column).astype(F32)
    back_rate = exact_dot(upper, back_cumulative)
    back_step = steps + back_rate * heads_ref[1:2, :]
    back_raw = back_step * sigmoid(raw)
    raw_ref[...] = back_raw.astype(BF)
    head_acc_ref[0:8, :] += jnp.sum(back_raw.reshape(CHUNK // 8, 8, LANES), axis=0)
    head_acc_ref[8:16, :] += jnp.sum((back_rate * rate).reshape(CHUNK // 8, 8, LANES), axis=0)


def constant(shape):
    return pl.BlockSpec(shape, lambda m, c: (0,) * len(shape))


def run_forward(x, tails, sraw, cols, segrow, taps, heads, spread, chunks):
    rows = x.shape[0]
    micro = rows // (chunks * CHUNK)
    flat = lambda width: pl.BlockSpec((CHUNK, width), lambda m, c: (m * chunks + c, 0))
    return pl.pallas_call(
        scan_forward,
        grid=(micro, chunks),
        in_specs=[
            flat(CHANNELS),
            pl.BlockSpec((1, 8, CHANNELS), lambda m, c: (m * chunks + c, 0, 0)),
            flat(LANES),
            flat(LANES),
            pl.BlockSpec((1, 8, LANES), lambda m, c: (m * chunks + c, 0, 0)),
            constant((8, CHANNELS)),
            constant((8, LANES)),
            constant((LANES, INNER)),
        ],
        out_specs=[
            flat(INNER),
            flat(INNER),
            flat(2 * STATE),
            flat(LANES),
            pl.BlockSpec((1, 1, STATE, INNER), lambda m, c: (m, c, 0, 0)),
            pl.BlockSpec((1, 1, 8, INNER), lambda m, c: (m, c, 0, 0)),
        ],
        out_shape=[
            jax.ShapeDtypeStruct((rows, INNER), F32),
            jax.ShapeDtypeStruct((rows, INNER), BF),
            jax.ShapeDtypeStruct((rows, 2 * STATE), BF),
            jax.ShapeDtypeStruct((rows, LANES), F32),
            jax.ShapeDtypeStruct((micro, chunks, STATE, INNER), BF),
            jax.ShapeDtypeStruct((micro, chunks, 8, INNER), F32),
        ],
        scratch_shapes=[pltpu.VMEM((STATE, INNER), F32), pltpu.VMEM((8, LANES), F32)],
        compiler_params=pltpu.CompilerParams(vmem_limit_bytes=VMEM_LIMIT),
        name="scan_forward",
    )(x, tails, sraw, cols, segrow, taps, heads, spread)


def run_backward(x, tails, sraw, cols, segrow, taps, heads, spread, gather, out, row_sums, states, decay, enter, back, chunks):
    rows = x.shape[0]
    micro = rows // (chunks * CHUNK)
    place = lambda m, c: m * chunks + chunks - 1 - c
    flat = lambda width: pl.BlockSpec((CHUNK, width), lambda m, c: (place(m, c), 0))
    return pl.pallas_call(
        scan_backward,
        grid=(micro, chunks),
        in_specs=[
            flat(CHANNELS),
            pl.BlockSpec((1, 8, CHANNELS), lambda m, c: (place(m, c), 0, 0)),
            flat(LANES),
            flat(LANES),
            pl.BlockSpec((1, 8, LANES), lambda m, c: (place(m, c), 0, 0)),
            constant((8, CHANNELS)),
            constant((8, LANES)),
            constant((LANES, INNER)),
            constant((INNER, LANES)),
            flat(INNER),
            flat(LANES),
            pl.BlockSpec((1, 1, STATE, INNER), lambda m, c: (m, jnp.maximum(chunks - 2 - c, 0), 0, 0)),
            pl.BlockSpec((1, 1, 8, INNER), lambda m, c: (m, jnp.maximum(chunks - 2 - c, 0), 0, 0)),
            pl.BlockSpec((1, STATE, INNER), lambda m, c: (m, 0, 0)),
            pl.BlockSpec((1, STATE, INNER), lambda m, c: (m, 0, 0)),
        ],
        out_specs=[
            flat(CHANNELS),
            flat(LANES),
            pl.BlockSpec((1, 8, CHANNELS), lambda m, c: (m, 0, 0)),
            constant((40, CHANNELS)),
            constant((16, LANES)),
        ],
        out_shape=[
            jax.ShapeDtypeStruct((rows, CHANNELS), BF),
            jax.ShapeDtypeStruct((rows, LANES), BF),
            jax.ShapeDtypeStruct((micro, 8, CHANNELS), BF),
            jax.ShapeDtypeStruct((40, CHANNELS), F32),
            jax.ShapeDtypeStruct((16, LANES), F32),
        ],
        scratch_shapes=[
            pltpu.VMEM((STATE, INNER), F32),
            pltpu.VMEM((TAPS - 1, 8, CHANNELS), F32),
        ],
        compiler_params=pltpu.CompilerParams(vmem_limit_bytes=VMEM_LIMIT),
        name="scan_backward",
    )(x, tails, sraw, cols, segrow, taps, heads, spread, gather, out, row_sums, states, decay, enter, back)


def fold(value):
    rows, lanes = value.shape
    return jnp.sum(value.reshape(rows // 8, 8, lanes), axis=0)


def mixer_kernel(
    core_ref,
    conv_ref,
    gate_ref,
    maps_ref,
    reach_ref,
    enter_ref,
    cols_ref,
    stream_ref,
    cot_ref,
    readout_ref,
    taps_ref,
    rescale_ref,
    spread_ref,
    gather_ref,
    result_ref,
    masked_ref,
    lifted_ref,
    out_ref,
    back_gate_ref,
    rows_ref,
    back_enter_ref,
    acc_ref,
    core_s,
    gated_s,
    silu_s,
    slope_s,
    back_s,
    reach_s,
    enter_s,
):
    rows = core_ref.shape[0]

    @pl.when((pl.program_id(0) == 0) & (pl.program_id(1) == 0))
    def _():
        acc_ref[...] = jnp.zeros_like(acc_ref)

    @pl.when(pl.program_id(1) == 0)
    def _():
        enter_s[...] = jnp.zeros_like(enter_s)

    reader = maps_ref[:, STATE:]
    reach2 = doubled(reach_ref[...])
    squares = jnp.zeros((rows, GROUP), F32)
    for group in range(INNER // GROUP):
        span = slice(group * GROUP, (group + 1) * GROUP)
        reach_x = nn(reach2, spread_ref[:, span])
        reach_s[:, span] = reach_x
        core = core_ref[:, span] + nn(reader, enter_ref[0, :, span]) * reach_x
        core_s[:, span] = core
        output = core + taps_ref[5:6, span] * conv_ref[:, span].astype(F32)
        gate = gate_ref[:, span].astype(F32)
        opened = sigmoid(gate)
        silu = gate * opened
        gated = output * silu
        gated_s[:, span] = gated
        silu_s[:, span] = silu
        slope_s[:, span] = output * opened * (1.0 + gate * (1.0 - opened))
        squares = squares + gated * gated
    inverse = lax.rsqrt(jnp.sum(squares, axis=1, keepdims=True) / INNER + EPS)
    for group in range(INNER // GROUP):
        span = slice(group * GROUP, (group + 1) * GROUP)
        lifted_ref[:, span] = (gated_s[:, span] * inverse * rescale_ref[0:1, span]).astype(BF)
    mixer = nt(lifted_ref[...], readout_ref[...])
    live = cols_ref[:, 6:7]
    result_ref[...] = (stream_ref[...].astype(F32) + live * mixer).astype(BF)
    masked = jnp.where(live > 0, cot_ref[...].astype(F32), 0.0).astype(BF)
    masked_ref[...] = masked
    terms = jnp.zeros((rows, GROUP), F32)
    for group in range(INNER // GROUP):
        span = slice(group * GROUP, (group + 1) * GROUP)
        back = nn(masked, readout_ref[:, span])
        product = back * gated_s[:, span]
        acc_ref[0:8, span] += fold(product * inverse)
        terms = terms + product * rescale_ref[0:1, span]
        back_s[:, span] = back * rescale_ref[0:1, span]
    dots = jnp.sum(terms, axis=1, keepdims=True)
    pull = inverse * inverse * inverse * (dots / INNER)
    reader_t = jnp.transpose(reader.astype(F32)).astype(BF)
    sums = jnp.zeros((rows, LANES), F32)
    for group in range(INNER // GROUP):
        span = slice(group * GROUP, (group + 1) * GROUP)
        back_gated = inverse * back_s[:, span] - gated_s[:, span] * pull
        out = (back_gated * silu_s[:, span]).astype(BF)
        out_ref[:, span] = out
        back_gate_ref[:, span] = (back_gated * slope_s[:, span]).astype(BF)
        out_f = out.astype(F32)
        acc_ref[8:16, span] += fold(out_f * conv_ref[:, span].astype(F32))
        high, low = pieces(out_f * core_s[:, span])
        sums = sums + nn(high, gather_ref[span, :]) + nn(low, gather_ref[span, :])
        enter_s[:, span] += nn(reader_t, (out_f * reach_s[:, span]).astype(BF))
    rows_ref[...] = sums
    back_enter_ref[0] = enter_s[...].astype(BF)


def run_mixer(core, convolved, gate, maps, reach, enter, cols, stream, cot, readout, taps, rescale, spread, gather, micro):
    total = core.shape[0]
    tile = min(256, total // micro)
    steps = total // micro // tile
    flat = lambda width: pl.BlockSpec((tile, width), lambda m, c: (m * steps + c, 0))
    state = pl.BlockSpec((1, STATE, INNER), lambda m, c: (m, 0, 0))
    wide_scratch = pltpu.VMEM((tile, INNER), F32)
    return pl.pallas_call(
        mixer_kernel,
        grid=(micro, steps),
        in_specs=[
            flat(INNER),
            flat(INNER),
            flat(INNER),
            flat(2 * STATE),
            flat(LANES),
            state,
            flat(LANES),
            flat(WIDTH),
            flat(WIDTH),
            constant((WIDTH, INNER)),
            constant((8, CHANNELS)),
            constant((8, INNER)),
            constant((LANES, INNER)),
            constant((INNER, LANES)),
        ],
        out_specs=[
            flat(WIDTH),
            flat(WIDTH),
            flat(INNER),
            flat(INNER),
            flat(INNER),
            flat(LANES),
            state,
            constant((16, INNER)),
        ],
        out_shape=[
            jax.ShapeDtypeStruct((total, WIDTH), BF),
            jax.ShapeDtypeStruct((total, WIDTH), BF),
            jax.ShapeDtypeStruct((total, INNER), BF),
            jax.ShapeDtypeStruct((total, INNER), BF),
            jax.ShapeDtypeStruct((total, INNER), BF),
            jax.ShapeDtypeStruct((total, LANES), F32),
            jax.ShapeDtypeStruct((micro, STATE, INNER), BF),
            jax.ShapeDtypeStruct((16, INNER), F32),
        ],
        scratch_shapes=[wide_scratch] * 6 + [pltpu.VMEM((STATE, INNER), F32)],
        compiler_params=pltpu.CompilerParams(vmem_limit_bytes=VMEM_LIMIT),
        name="gated_mixer",
    )(core, convolved, gate, maps, reach, enter, cols, stream, cot, readout, taps, rescale, spread, gather)

MESH = pl.DeviceIdType.MESH


def places():
    dp = lax.axis_index("dp")
    tensor = lax.axis_index("tensor")
    return {"Z": dp // 8, "z": (dp // 4) % 2, "x": (dp // 2) % 2, "c": dp % 2, "t": tensor}


def partner(at, axis):
    to = dict(at)
    to[axis] = 1 - at[axis]
    return (to["Z"] * 8 + to["z"] * 4 + to["x"] * 2 + to["c"], to["t"])


def greet(at):
    barrier = pltpu.get_barrier_semaphore()
    for axis in ("Z", "z", "x", "c", "t"):
        pl.semaphore_signal(barrier, inc=1, device_id=partner(at, axis), device_id_type=MESH)
    pl.semaphore_wait(barrier, 5)


GATHER_ORDERS = (("Z", "z", "x", "t", "c"), ("Z", "z", "t", "x", "c"))
SCATTER_ORDERS = (("c", "t", "x", "z", "Z"), ("c", "x", "t", "z", "Z"))
AXES = ("Z", "z", "x", "t")
HALF = INNER // 4
SMALL = ("small", 0)
SELECT = ("select", 0)
CHAINS = (SMALL, (0, 0), (0, 1), SELECT, (1, 0), (1, 1), (2, 0), (2, 1))
DELAYS = (0, 0, 0, 0, 1, 1, 2, 2)


def half_lanes(tensor, half):
    return pl.ds(pl.multiple_of(tensor * (INNER // 2) + half * HALF, LANES), HALF)


def order_of(chain, orders):
    return orders[1] if chain == SMALL else orders[chain[1]]


def gather_kernel(main_ref, select_ref, small_ref, whole_ref, selects_ref, smalls_ref, send, recv, own):
    at = places()
    greet(at)

    def source(chain):
        piece, half = chain
        if chain == SELECT:
            return select_ref
        if chain == SMALL:
            return small_ref
        return main_ref.at[piece, :, half * HALF : (half + 1) * HALF]

    def views(chain, done):
        piece, half = chain
        index = tuple(slice(None) if axis in done else at[axis] for axis in ("Z", "z", "x", "c"))
        tensors = range(2) if "t" in done else [at["t"]]
        if chain in (SELECT, SMALL):
            whole = selects_ref if chain == SELECT else smalls_ref
            return [whole.at[index + (slice(None) if "t" in done else at["t"],)]]
        return [whole_ref.at[(piece,) + index + (slice(None), half_lanes(tensor, half))] for tensor in tensors]

    copies = []
    for number, chain in enumerate(CHAINS):
        copy = pltpu.make_async_copy(source(chain), views(chain, ())[0], own.at[number])
        copy.start()
        copies.append(copy)
    flights = {}
    for tick in range(5 + max(DELAYS)):
        for number, chain in enumerate(CHAINS):
            stage = tick - DELAYS[number]
            if not 0 <= stage < 5:
                continue
            order = order_of(chain, GATHER_ORDERS)
            targets = views(chain, order[:stage])
            if stage == 0:
                origins = [source(chain)]
            else:
                if stage == 1:
                    copies[number].wait()
                for flight in flights[number, stage - 1]:
                    flight.wait_recv()
                origins = targets
            flights[number, stage] = []
            for index, (origin, target) in enumerate(zip(origins, targets)):
                flight = pltpu.make_async_remote_copy(
                    src_ref=origin,
                    dst_ref=target,
                    send_sem=send.at[number, stage * 2 + index],
                    recv_sem=recv.at[number, stage * 2 + index],
                    device_id=partner(at, order[stage]),
                    device_id_type=MESH,
                )
                flight.start()
                flights[number, stage].append(flight)
    for (number, stage), group in flights.items():
        for flight in group:
            if stage == 4:
                flight.wait_recv()
            flight.wait_send()


def gather_fast(main, select, small):
    anywhere = pl.BlockSpec(memory_space=pl.ANY)
    inside = pl.BlockSpec(memory_space=pltpu.VMEM)
    return pl.pallas_call(
        gather_kernel,
        in_specs=[inside] * 3,
        out_specs=[anywhere] * 3,
        out_shape=[
            jax.ShapeDtypeStruct((3, 2, 2, 2, 2, 48, INNER), BF),
            jax.ShapeDtypeStruct((2, 2, 2, 2, 2, 24, 2 * STATE), BF),
            jax.ShapeDtypeStruct((2, 2, 2, 2, 2, 8, LANES), F32),
        ],
        scratch_shapes=[
            pltpu.SemaphoreType.DMA((8, 10)),
            pltpu.SemaphoreType.DMA((8, 10)),
            pltpu.SemaphoreType.DMA((8,)),
        ],
        compiler_params=pltpu.CompilerParams(collective_id=0, has_side_effects=True),
        name="gather_weights",
    )(main, select, small)


BUFFERS = 10


def scatter_kernel(*refs):
    grads, selects_ref, smalls_ref = refs[0:3], refs[3], refs[4]
    main_out, select_out, small_out = refs[5:8]
    send, recv, own = refs[8:11]
    buffers = refs[11:]
    at = places()
    greet(at)

    def sources(chain, core, target):
        piece, half = chain
        if chain in (SELECT, SMALL):
            whole = selects_ref if chain == SELECT else smalls_ref
            return [(whole.at[:, :, :, core], target)]
        return [
            (grads[piece].at[:, :, :, core, :, half_lanes(tensor, half)], target.at[:, :, :, tensor])
            for tensor in range(2)
        ]

    copies = {}
    for number, chain in enumerate(CHAINS):
        copies[number] = []
        for index, (origin, target) in enumerate(sources(chain, at["c"], buffers[number * BUFFERS])):
            copy = pltpu.make_async_copy(origin, target, own.at[number, index])
            copy.start()
            copies[number].append(copy)
    flights = {}

    def start(number, stage):
        chain = CHAINS[number]
        order = order_of(chain, SCATTER_ORDERS)
        arrived = buffers[number * BUFFERS + 1 + 2 * stage]
        if stage == 0:
            parts = sources(chain, 1 - at["c"], arrived)
        else:
            remaining = [axis for axis in AXES if axis not in order[1:stage]]
            position = remaining.index(order[stage])
            held = buffers[number * BUFFERS + 2 * stage]
            parts = [(held.at[(slice(None),) * position + (1 - at[order[stage]],)], arrived)]
        flights[number, stage] = []
        for index, (origin, target) in enumerate(parts):
            flight = pltpu.make_async_remote_copy(
                src_ref=origin,
                dst_ref=target,
                send_sem=send.at[number, stage * 2 + index],
                recv_sem=recv.at[number, stage * 2 + index],
                device_id=partner(at, order[stage]),
                device_id_type=MESH,
            )
            flight.start()
            flights[number, stage].append(flight)

    def finish(number, stage):
        chain = CHAINS[number]
        order = order_of(chain, SCATTER_ORDERS)
        for flight in flights[number, stage]:
            flight.wait_recv()
        arrived = buffers[number * BUFFERS + 1 + 2 * stage]
        if stage == 0:
            for copy in copies[number]:
                copy.wait()
            mine, target = buffers[number * BUFFERS], buffers[number * BUFFERS + 2]
            for index in range(8):
                where = (index // 4, (index // 2) % 2, index % 2)
                target[where] = (mine[where].astype(F32) + arrived[where].astype(F32)).astype(target.dtype)
            return
        remaining = [axis for axis in AXES if axis not in order[1:stage]]
        position = remaining.index(order[stage])
        held = buffers[number * BUFFERS + 2 * stage]
        chosen = held[(slice(None),) * position + (at[order[stage]],)]
        total = chosen.astype(F32) + arrived[...].astype(F32)
        if stage < 4:
            target = buffers[number * BUFFERS + 2 + 2 * stage]
            target[...] = total.astype(target.dtype)
        elif chain == SELECT:
            select_out[...] = total
        elif chain == SMALL:
            small_out[...] = total
        else:
            main_out[chain[0], :, chain[1] * HALF : (chain[1] + 1) * HALF] = total

    for tick in range(6 + max(DELAYS)):
        for number in range(len(CHAINS)):
            stage = tick - DELAYS[number]
            if 0 < stage <= 5:
                finish(number, stage - 1)
            if 0 <= stage < 5:
                start(number, stage)
    for group in flights.values():
        for flight in group:
            flight.wait_send()


def scatter_fast(first, second, third, select, small):
    anywhere = pl.BlockSpec(memory_space=pl.ANY)
    inside = pl.BlockSpec(memory_space=pltpu.VMEM)
    scratch = [
        pltpu.SemaphoreType.DMA((8, 10)),
        pltpu.SemaphoreType.DMA((8, 10)),
        pltpu.SemaphoreType.DMA((8, 2)),
    ]
    for chain in CHAINS:
        block, kind = (48, HALF), BF
        if chain == SELECT:
            block = (24, 2 * STATE)
        if chain == SMALL:
            block, kind = (8, LANES), F32
        for depth in (4, 4, 4, 3, 3, 2, 2, 1, 1, 0):
            scratch.append(pltpu.VMEM((2,) * depth + block, kind))
    return pl.pallas_call(
        scatter_kernel,
        in_specs=[anywhere] * 5,
        out_specs=[inside] * 3,
        out_shape=[
            jax.ShapeDtypeStruct((3, 48, INNER // 2), F32),
            jax.ShapeDtypeStruct((24, 2 * STATE), F32),
            jax.ShapeDtypeStruct((8, LANES), F32),
        ],
        scratch_shapes=scratch,
        compiler_params=pltpu.CompilerParams(
            collective_id=1, has_side_effects=True, vmem_limit_bytes=VMEM_LIMIT
        ),
        name="scatter_gradients",
    )(first, second, third, select, small)


def gather_weights(shards):
    flat = jnp.concatenate([shard.reshape(-1) for shard in shards])
    everyone = lax.all_gather(flat, ("dp", "tensor"), axis=0, tiled=False)
    everyone = everyone.reshape(lax.axis_size("dp"), lax.axis_size("tensor"), flat.shape[0])
    result = []
    start = 0
    for shard in shards:
        result.append(everyone[:, :, start : start + shard.size].reshape(everyone.shape[:2] + shard.shape))
        start += shard.size
    return result


def join(shards, dp_dim, tensor_dim):
    groups, members = shards.shape[:2]
    shape = list(shards.shape[2:])
    order = []
    for dim in range(len(shape)):
        if dim == dp_dim:
            order.append(0)
        if dim == tensor_dim:
            order.append(1)
        order.append(dim + 2)
    full = shape[:]
    full[dp_dim] *= groups
    full[tensor_dim] *= members
    return jnp.transpose(shards, order).reshape(full)


def cut(full, dp_dim, tensor_dim):
    groups, members = lax.axis_size("dp"), lax.axis_size("tensor")
    shape = []
    for dim, size in enumerate(full.shape):
        if dim == dp_dim:
            shape.append(groups)
            size //= groups
        if dim == tensor_dim:
            shape.append(members)
            size //= members
        shape.append(size)
    both = full.reshape(shape)
    position = dp_dim + (1 if tensor_dim < dp_dim else 0)
    where = tensor_dim + (1 if dp_dim <= tensor_dim else 0)
    return jnp.moveaxis(both, (position, where), (0, 1))


def reduce_shards(grads, places, shapes):
    groups, members = lax.axis_size("dp"), lax.axis_size("tensor")
    flat = jnp.concatenate(
        [cut(grad.astype(BF), *place).reshape(groups * members, -1) for grad, place in zip(grads, places)], axis=1
    )
    mine = lax.psum_scatter(flat, ("dp", "tensor"), scatter_dimension=0, tiled=True).reshape(-1).astype(F32)
    result = []
    start = 0
    for shape in shapes:
        size = 1
        for extent in shape:
            size *= extent
        result.append(mine[start : start + size].reshape(shape))
        start += size
    return result


def chain(own, decay, forward):
    members = lax.axis_size("tensor")
    if forward:
        hops = [(index, index + 1) for index in range(members - 1)]
    else:
        hops = [(index + 1, index) for index in range(members - 1)]
    held = None
    for _ in range(members - 1):
        value = own if held is None else own + decay * held.astype(F32)
        held = lax.ppermute(value.astype(BF), "tensor", hops)
    return held


def marks(bounds, rows, chunks):
    place = lax.axis_index("tensor")
    local = jnp.arange(rows, dtype=jnp.int32)[None, :]
    position = local + place * rows
    first = bounds[:, 0, 0:1]
    used = bounds[:, 0, 1:2]

    def segment_at(where):
        value = (where >= first).astype(jnp.int32) + (where >= used).astype(jnp.int32)
        return jnp.where(where < 0, -1, value)

    segment = segment_at(position)
    start = position - local % CHUNK
    columns = [segment == segment_at(position - back) for back in range(1, TAPS)]
    columns.append(segment == segment_at(start - 1))
    columns.append(segment == segment_at(start + CHUNK - 1))
    columns.append(segment)
    columns.append(position < used)
    columns.append(segment == segment_at(position * 0 + place * rows - 1))
    lane = lax.broadcasted_iota(jnp.int32, (1, 1, LANES), 2)
    table = jnp.zeros(segment.shape + (LANES,), F32)
    for index, column in enumerate(columns):
        table = jnp.where(lane == index, column.astype(F32)[:, :, None], table)
    across = jnp.broadcast_to(
        segment.astype(F32).reshape(-1, 1, CHUNK), (segment.shape[0] * chunks, 8, CHUNK)
    )
    return table.reshape(-1, LANES), across


def local(
    stream,
    bounds,
    prescale,
    expansion,
    timestep,
    selection,
    kernels,
    biases,
    stencil,
    baseline,
    offset,
    decays,
    passthrough,
    rescale,
    readout,
    cotangent,
):
    members = lax.axis_size("tensor")
    place = lax.axis_index("tensor")
    micro, rows = stream.shape[:2]
    chunks = rows // CHUNK
    assert rows * members == SLOT and bounds.shape[1] == 1
    fast = members == 2 and lax.axis_size("dp") == 16 and expansion.shape == (48, 2, 768)
    small = (timestep, kernels, biases, rescale, prescale, stencil, baseline, offset, decays, passthrough)
    if fast:
        main = jnp.concatenate([jnp.swapaxes(expansion, 0, 1), readout.T[None]], axis=0)
        packed = jnp.concatenate([item.reshape(-1).astype(F32) for item in small])
        packed = jnp.pad(packed, (0, 8 * LANES - packed.shape[0])).reshape(8, LANES)
        main, select, packed = gather_fast(main, selection, packed)
        main = main.reshape(3, WIDTH, INNER)
        gate_weight, inner_weight, readout_t = main[0], main[1], main[2]
        select = select.reshape(WIDTH, 2 * STATE)
        packed = packed.reshape(16, 2, 8 * LANES)
        got = []
        start = 0
        for item in small:
            got.append(packed[:, :, start : start + item.size].reshape((16, 2) + item.shape))
            start += item.size
    else:
        got = gather_weights(small + (expansion, selection, readout))
        expand = join(got[10], 0, 2)
        gate_weight, inner_weight = expand[:, 0, :], expand[:, 1, :]
        select = got[11].reshape(WIDTH, 2 * STATE)
        readout_t = join(got[12], 1, 0).T
    time_full = join(got[0], 0, 1).astype(BF)
    kernel_full = join(got[1], 1, 0).reshape(INNER, TAPS)
    bias_full = join(got[2], 1, 0).reshape(INNER)
    rescale_full = join(got[3], 1, 0).reshape(1, INNER).astype(F32)
    prescale_full = got[4].reshape(WIDTH).astype(F32)
    stencil_full = got[5].reshape(2 * STATE, TAPS)
    baseline_full = got[6].reshape(2 * STATE)
    offset_full, decays_full, pass_full = (item[0].reshape(HEADS).astype(F32) for item in got[7:10])

    head = lax.broadcasted_iota(jnp.int32, (LANES, INNER), 0)
    channel = lax.broadcasted_iota(jnp.int32, (LANES, INNER), 1) // HEAD_DIM
    spread = ((head < 2 * HEADS) & (head % HEADS == channel)).astype(BF)
    gather = ((head < HEADS) & (head == channel)).astype(BF).T
    pass_wide = jnp.repeat(pass_full, HEAD_DIM)
    taps = jnp.concatenate([kernel_full, stencil_full], axis=0).astype(F32).T
    shifts = jnp.concatenate([bias_full, baseline_full]).astype(F32)[None]
    last = jnp.concatenate([pass_wide, jnp.zeros((2 * STATE,), F32)])[None]
    taps = jnp.concatenate([taps, shifts, last, jnp.zeros((2, CHANNELS), F32)], axis=0)
    heads = jnp.pad(jnp.stack([offset_full, -jnp.exp(decays_full)]), ((0, 6), (0, LANES - HEADS)))
    cols, segrow = marks(bounds, rows, chunks)

    flat = stream.reshape(micro * rows, WIDTH)

    def low_norm(values):
        values = values.astype(F32)
        return (values * lax.rsqrt(jnp.mean(values * values, axis=-1, keepdims=True) + EPS) * prescale_full).astype(BF)

    hops = [(index, index + 1) for index in range(members - 1)]
    edge = lax.ppermute(stream[:, rows - 8 :, :], "tensor", hops).reshape(micro * 8, WIDTH)
    lowered = low_norm(flat)
    lowered_edge = low_norm(edge)
    signal_weight = jnp.concatenate([inner_weight, select], axis=1)
    time_weight = jnp.pad(time_full, ((0, 0), (0, LANES - HEADS)))
    signal = nn(lowered, signal_weight).astype(BF)
    signal_edge = nn(lowered_edge, signal_weight).astype(BF)
    gate = nn(lowered, gate_weight).astype(BF)
    sraw = nn(lowered, time_weight)
    tails = jnp.concatenate(
        [
            signal_edge.reshape(micro, 1, 8, CHANNELS),
            signal.reshape(micro, chunks, CHUNK, CHANNELS)[:, : chunks - 1, CHUNK - 8 :, :],
        ],
        axis=1,
    ).reshape(micro * chunks, 8, CHANNELS)
    core, convolved, maps, reach, states, decay = run_forward(
        signal, tails, sraw, cols, segrow, taps, heads, spread, chunks
    )
    total_decay = decay[:, chunks - 1, 0:1, :]
    enter = chain(states[:, chunks - 1].astype(F32), total_decay, True)

    cot = cotangent.reshape(micro * rows, WIDTH)
    result, masked, lifted, out, back_gate, row_sums, back_enter, mix_acc = run_mixer(
        core,
        convolved,
        gate,
        maps,
        reach,
        enter,
        cols,
        flat,
        cot,
        readout_t,
        taps,
        jnp.broadcast_to(rescale_full, (8, INNER)),
        spread,
        gather,
        micro,
    )
    readout_term = tn(masked, lifted).astype(BF)
    back = chain(back_enter.astype(F32), total_decay, False)

    grad_signal, back_raw, halo, acc, head_acc = run_backward(
        signal, tails, sraw, cols, segrow, taps, heads, spread, gather, out, row_sums, states, decay, enter, back, chunks
    )
    returned = lax.ppermute(halo, "tensor", [(index + 1, index) for index in range(members - 1)])
    grad_signal = grad_signal.reshape(micro, rows, CHANNELS)
    fixed = (grad_signal[:, rows - 8 :].astype(F32) + returned.astype(F32)).astype(BF)
    grad_signal = lax.dynamic_update_slice_in_dim(grad_signal, fixed, rows - 8, 1).reshape(micro * rows, CHANNELS)

    gate_term = tn(lowered, back_gate).astype(BF)
    inner_term = tn(lowered, grad_signal[:, :INNER]).astype(BF)
    select_term = tn(lowered, grad_signal[:, INNER:]).astype(BF)
    time_term = tn(lowered, back_raw)[:, :HEADS]
    back_lowered = nt(back_gate, gate_weight) + nt(grad_signal, signal_weight) + nt(back_raw, time_weight)
    values = flat.astype(F32)
    scale = lax.rsqrt(jnp.mean(values * values, axis=-1, keepdims=True) + EPS)
    prescale_term = jnp.sum(back_lowered * values * scale, axis=0)
    held = back_lowered * prescale_full
    grad_stream = held * scale - values * (scale * scale * scale) * jnp.mean(held * values, axis=-1, keepdims=True)
    grad_stream = (cot.astype(F32) + grad_stream).astype(BF)

    sums = jnp.sum(acc.reshape(5, 8, CHANNELS), axis=1)
    tap_terms = jnp.stack([sums[4], sums[3], sums[2], sums[1]], axis=1)
    head_sums = jnp.sum(head_acc.reshape(2, 8, LANES), axis=1)[:, :HEADS]
    mix_sums = jnp.sum(mix_acc.reshape(2, 8, INNER), axis=1)
    small_grads = (
        (time_term, (0, 1)),
        (tap_terms[:INNER].reshape(HEADS, HEAD_DIM * TAPS), (1, 0)),
        (sums[0, :INNER].reshape(HEADS, HEAD_DIM), (1, 0)),
        (mix_sums[0].reshape(HEADS, HEAD_DIM), (1, 0)),
        (prescale_term, (0, 0)),
        (tap_terms[INNER:], (0, 0)),
        (sums[0, INNER:], (0, 0)),
    )
    scalars = jnp.stack([head_sums[0], head_sums[1], jnp.sum(mix_sums[1].reshape(HEADS, HEAD_DIM), axis=1)])
    shapes = [item.shape for item in small]
    if fast:
        scalars = jnp.swapaxes(scalars.reshape(3, 2, HEADS // 2), 0, 1).reshape(1, 2, -1)
        packed = jnp.concatenate(
            [cut(grad, *where).reshape(16, 2, -1) for grad, where in small_grads]
            + [jnp.broadcast_to(scalars, (16,) + scalars.shape[1:])],
            axis=2,
        )
        packed = jnp.pad(packed, ((0, 0), (0, 0), (0, 8 * LANES - packed.shape[2])))
        square = lambda grad: grad.reshape(2, 2, 2, 2, 48, INNER)
        main, select_grad, packed = scatter_fast(
            square(readout_term),
            square(gate_term),
            square(inner_term),
            select_term.reshape(2, 2, 2, 2, 2, 24, 2 * STATE),
            packed.reshape(2, 2, 2, 2, 2, 8, LANES),
        )
        expansion_grad = jnp.stack([main[1], main[2]], axis=1)
        readout_grad = main[0].T
        packed = packed.reshape(-1)
        done = []
        start = 0
        for item in small:
            done.append(packed[start : start + item.size].reshape(item.shape))
            start += item.size
    else:
        grads = [grad for grad, _ in small_grads] + [
            jnp.stack([gate_term, inner_term], axis=1),
            select_term,
            readout_term.T,
        ]
        wheres = [where for _, where in small_grads] + [(0, 2), (0, 0), (1, 0)]
        done = reduce_shards(grads, wheres, shapes[:7] + [expansion.shape, selection.shape, readout.shape])
        expansion_grad, select_grad, readout_grad = done[7:]
        scalars = lax.psum(scalars, ("dp", "tensor"))
        scalars = lax.dynamic_slice_in_dim(scalars, place * offset.shape[0], offset.shape[0], axis=1)
        done = done[:7] + [scalars[0], scalars[1], scalars[2]]
    return (
        result.reshape(stream.shape),
        grad_stream.reshape(stream.shape),
        done[4],
        expansion_grad,
        done[0],
        select_grad,
        done[1],
        done[2],
        done[5],
        done[6],
        done[7],
        done[8],
        done[9],
        done[3],
        readout_grad,
    )


def solution(mesh):
    everything = ("dp", "tensor")
    rows = P(None, everything, None)
    weights = (
        P(everything),
        P("dp", None, "tensor"),
        P("dp", "tensor"),
        P(everything, None),
        P("tensor", "dp"),
        P("tensor", "dp"),
        P(everything, None),
        P(everything),
        P("tensor"),
        P("tensor"),
        P("tensor"),
        P("tensor", "dp"),
        P("tensor", "dp"),
    )
    return jax.shard_map(
        local,
        mesh=mesh,
        in_specs=(rows, P(None, "dp", None)) + weights + (rows,),
        out_specs=(rows, rows) + weights,
        check_vma=False,
    )
```
